32 devices in a mesh: bank: 8 (over z, core), zero: 4 (over y, x).
Axes of the slice: x: 2, y: 2, z: 4, core: 2. Of those that a mesh axis runs over, the one named last changes fastest.
Arguments:
- w_down: float32 [64, 1024, 2048], P('bank', None, 'zero'), may hold values from -0.25 to 0.25
- avg_down: float32 [64, 1024, 2048], P('bank', None, 'zero'), may hold values from -0.1875 to 0.1875
- mix_share: float32 [64], P('bank'), may hold values from 0.2 to 0.8
- router_weight: float32 [2048, 64], P('zero', 'bank'), may hold values from -0.125 to 0.125
- router_gain: float32 [2048], P('zero'), may hold values from 0.25 to 1.75
Outputs:
- serve_down: bfloat16 [64, 1024, 2048], P('bank')
- scale_down: float32 [64, 1024], P('bank')
- serve_router: bfloat16 [2048, 64], replicated
The draws below stay inside these ranges and needn't reach their ends.
All inputs are finite; a program needn't handle non-finite values. Where the reference program divides by a largest or mean magnitude, that divisor is 1e-20 or more.
Results may differ from the reference program's by a relative error of at most 0.001.
Values may be sent and summed in bfloat16 or wider, within the bound.
A program may use at most 192 MiB of HBM per device.

```python
import jax
import jax.numpy as jnp

EXPERTS = 64
D_MODEL = 2048
D_EXPERT = 1024


def raised(values, stream_key, source, target, shards_of, factor):
    def block_of(axis_at):
        return (jnp.arange(values.shape[axis_at]) // (values.shape[axis_at] // shards_of)).reshape((-1,) + (1,) * (values.ndim - 1 - axis_at))

    near = jax.random.permutation(stream_key, shards_of)[block_of(target)]
    other_side = (block_of(target) + shards_of // 2) % shards_of
    return jnp.where((block_of(source) == near) | (block_of(source) == other_side), factor * values, values)


def shard_levels(key, extent, split, low, high):
    gain, own = 1.0, jax.random.fold_in(key, 6)
    for dim, blocks in split:
        draws = jnp.exp(jax.random.uniform(jax.random.fold_in(own, dim), (blocks,), jnp.float32, low / len(split), high / len(split)))
        gain = gain * jnp.repeat(draws, extent[dim] // blocks).reshape([-1 if axis == dim else 1 for axis in range(len(extent))])
    return gain


def centred(own_key, extent, spread, limit, shards=(), kind=jnp.bfloat16):
    result = jax.random.normal(own_key, extent, jnp.float32) * spread
    if len(shards) > 0:
        result = shard_levels(own_key, extent, shards, -0.22, 0.18) * result
    return jnp.clip(result, min=-limit, max=limit).astype(kind)


def bell_draw_with(rng, dims, width, bound, shards, heavy, kind=jnp.bfloat16):
    drawn = width * jax.random.normal(rng, dims, jnp.float32)
    if shards:
        drawn = drawn * shard_levels(rng, dims, shards, -0.22, 0.18)
    return jnp.clip(raised(drawn, jax.random.fold_in(rng, 3), *heavy), -bound, bound).astype(kind)


def setup_inputs(seed: int = 0) -> dict:
    arg_keys = jax.random.split(jax.random.key(seed), 6)
    return {
        "w_down": bell_draw_with(arg_keys[0], (EXPERTS, D_EXPERT, D_MODEL), D_EXPERT ** -0.5, 0.25, ((0, 8), (2, 4)), (2, 1, 4, 2.0), jnp.float32),
        "avg_down": centred(arg_keys[1], (EXPERTS, D_EXPERT, D_MODEL), D_EXPERT ** -0.5, 0.1875, ((0, 8), (2, 4)), jnp.float32),
        "mix_share": jnp.clip(0.2 + 0.6 * jax.random.uniform(arg_keys[2], (EXPERTS,), jnp.float32) ** shard_levels(arg_keys[2], (EXPERTS,), ((0, 8),), -0.2, 0.2), 0.2, 0.8),
        "router_weight": centred(arg_keys[3], (D_MODEL, EXPERTS), D_MODEL ** -0.5, 0.125, ((0, 4), (1, 8)), jnp.float32),
        "router_gain": jnp.clip(1.0 + 0.15 * jax.random.normal(arg_keys[4], (D_MODEL,), jnp.float32), 0.25, 1.75),
    }


def reference(w_down, avg_down, mix_share, router_weight, router_gain):
    fresh_down = mix_share[:, None, None] * w_down + (1.0 - mix_share[:, None, None]) * avg_down
    scale_down = jnp.max(jnp.abs(fresh_down), axis=2)
    serve_down = (fresh_down / jnp.expand_dims(scale_down, 2)).astype(jnp.bfloat16)
    serve_router = (router_weight * router_gain[:, None]).astype(jnp.bfloat16)
    return serve_down, scale_down, serve_router
```

```python
import functools

import jax
import jax.numpy as jnp
from jax import lax
from jax.experimental import pallas as pl
from jax.experimental.pallas import tpu as pltpu
from jax.sharding import PartitionSpec as P

MESH = pl.DeviceIdType.MESH
LANES = 128
ROWS = 512
TAIL_EXPERTS = 2
IN_SLOTS = 3


def peers_of(zero):
    side = lax.rem(zero, 2)
    return zero + 1 - 2 * side, lax.rem(zero + 2, 4), 3 - zero


def exchange_kernel(
    banks, chunks, rows, tail,
    w_hbm, a_hbm, mix, router_t, gain,
    full, tail_x, tail_y, scale_out, router_out,
    w_buf, a_buf, fresh, narrow, own_max, peer_max, scales, router_buf,
    in_sem, max_send, max_recv, send_x, send_y, send_f, recv_x, recv_y, recv_d,
    keep_sem, tail_sem, bank_send, bank_recv, square_send, square_recv,
):
    zero, bank = lax.axis_index("zero"), lax.axis_index("bank")
    square = peers_of(zero)
    px, py, pd = square
    per = w_hbm.shape[1] // rows
    width = w_hbm.shape[2]
    blocks = rows // LANES
    groups = width // LANES

    def place(c, owner):
        cols = pl.ds(pl.multiple_of(owner * width, width), width)
        return full.at[lax.div(c, per), pl.ds(pl.multiple_of(lax.rem(c, per) * rows, rows), rows), cols]

    def loads(c):
        slot = lax.rem(c, IN_SLOTS)
        piece = (lax.div(c, per), pl.ds(pl.multiple_of(lax.rem(c, per) * rows, rows), rows))
        return (
            pltpu.make_async_copy(w_hbm.at[piece], w_buf.at[slot], in_sem.at[0, slot]),
            pltpu.make_async_copy(a_hbm.at[piece], a_buf.at[slot], in_sem.at[1, slot]),
        )

    def start_loads(c):
        for copy in loads(c):
            copy.start()

    def remote(src, dst, send, recv, to):
        return pltpu.make_async_remote_copy(
            src_ref=src, dst_ref=dst, send_sem=send, recv_sem=recv,
            device_id={"zero": to}, device_id_type=MESH,
        )

    def max_copy(c, k):
        return remote(own_max.at[c], peer_max.at[k, c], max_send.at[k, c], max_recv.at[k, c], square[k])

    def to_x(c, owner):
        return remote(narrow.at[c], place(c, owner), send_x.at[c], recv_x.at[c], px)

    def to_y(c, owner):
        return remote(narrow.at[c], place(c, owner), send_y.at[c], recv_y.at[c], py)

    def on_x(c):
        return (c < chunks - tail) | (lax.rem(c, 2) == 0)

    def on_y(c):
        return (c < chunks - tail) | (lax.rem(c, 2) == 1)

    def keep(c):
        return pltpu.make_async_copy(narrow.at[c], place(c, zero), keep_sem.at[c])

    def mix_stage(c):
        for copy in loads(c):
            copy.wait()

        @pl.when(c + IN_SLOTS - 1 < chunks)
        def _():
            start_loads(c + IN_SLOTS - 1)

        slot, half = lax.rem(c, IN_SLOTS), lax.rem(c, 2)
        share = mix[lax.div(c, per)]
        for j in range(blocks):
            part = pl.ds(j * LANES, LANES)
            value = share * w_buf[slot, part, :] + (1.0 - share) * a_buf[slot, part, :]
            fresh[half, part, :] = value
            size = jnp.abs(value)
            top = size[:, :LANES]
            for g in range(1, groups):
                top = jnp.maximum(top, size[:, g * LANES:(g + 1) * LANES])
            own_max[c, pl.ds(j, 1), :] = jnp.max(top.T, axis=0, keepdims=True)
        for k in range(3):
            max_copy(c, k).start()

    def send_stage(c):
        for k in range(3):
            max_copy(c, k).wait_recv()
        scale = jnp.maximum(
            jnp.maximum(own_max[c], peer_max[0, c]), jnp.maximum(peer_max[1, c], peer_max[2, c])
        )
        scales[c] = scale
        inverse = 1.0 / scale
        half = lax.rem(c, 2)
        for j in range(blocks):
            part = pl.ds(j * LANES, LANES)
            column = jnp.broadcast_to(inverse[j:j + 1, :], (LANES, LANES)).T
            for g in range(groups):
                cols = slice(g * LANES, (g + 1) * LANES)
                narrow[c, part, cols] = (fresh[half, part, cols] * column).astype(narrow.dtype)

        @pl.when(on_x(c))
        def _():
            to_x(c, zero).start()

        @pl.when(on_y(c))
        def _():
            to_y(c, zero).start()

        keep(c).start()

    def forward(c, do):
        @pl.when(lax.rem(c, 2) == 0)
        def _():
            do(remote(place(c, px), place(c, px), send_f.at[c], recv_d.at[c], py))

        @pl.when(lax.rem(c, 2) == 1)
        def _():
            do(remote(place(c, py), place(c, py), send_f.at[c], recv_d.at[c], px))

    for c in range(IN_SLOTS - 1):
        start_loads(c)
    barrier = pltpu.get_barrier_semaphore()
    others = [lax.rem(bank + k, banks) for k in range(1, banks)]
    for to in square:
        pl.semaphore_signal(barrier, inc=1, device_id={"zero": to}, device_id_type=MESH)
    for to in others:
        pl.semaphore_signal(barrier, inc=1, device_id={"bank": to}, device_id_type=MESH)
    pl.semaphore_wait(barrier, 3 + len(others))

    mix_stage(0)

    def main(c, carry):
        mix_stage(c)
        send_stage(c - 1)
        return carry

    lax.fori_loop(1, chunks, main, 0)
    send_stage(chunks - 1)

    tails = []
    for n in range(tail):
        c = chunks - tail + n
        out = tail_y if c % 2 == 0 else tail_x
        tails.append(pltpu.make_async_copy(narrow.at[c], out.at[n // 2], tail_sem.at[n]))
        tails[-1].start()

    router_buf[zero, bank] = (router_t[...] * gain[...]).astype(router_buf.dtype)
    bank_copies = [
        pltpu.make_async_remote_copy(
            src_ref=router_buf.at[zero, bank], dst_ref=router_buf.at[zero, bank],
            send_sem=bank_send.at[k], recv_sem=bank_recv.at[k],
            device_id={"bank": to}, device_id_type=MESH,
        )
        for k, to in enumerate(others)
    ]
    for copy in bank_copies:
        copy.start()
    for k in range(len(others)):
        source = lax.rem(bank + banks - k - 1, banks)
        pltpu.make_async_remote_copy(
            src_ref=router_buf.at[zero, source], dst_ref=router_buf.at[zero, source],
            send_sem=bank_send.at[k], recv_sem=bank_recv.at[k],
            device_id={"bank": others[k]}, device_id_type=MESH,
        ).wait_recv()
    square_copies = [
        remote(router_buf.at[zero], router_buf.at[zero], square_send.at[k], square_recv.at[k], square[k])
        for k in range(3)
    ]
    for copy in square_copies:
        copy.start()

    def relay(c, carry):
        @pl.when(lax.rem(c, 2) == 0)
        def _():
            to_x(c, px).wait_recv()

        @pl.when(lax.rem(c, 2) == 1)
        def _():
            to_y(c, py).wait_recv()

        forward(c, lambda copy: copy.start())
        return carry

    lax.fori_loop(0, chunks, relay, 0)

    for c in range(chunks):
        scale_out[c // per:c // per + 1, pl.ds((c % per) * rows, rows)] = jnp.concatenate(
            [scales[c, j:j + 1, :] for j in range(blocks)], axis=1
        )

    def settle(c, carry):
        @pl.when((lax.rem(c, 2) == 1) & (c < chunks - tail))
        def _():
            to_x(c, px).wait_recv()

        @pl.when((lax.rem(c, 2) == 0) & (c < chunks - tail))
        def _():
            to_y(c, py).wait_recv()

        @pl.when(on_x(c))
        def _():
            to_x(c, zero).wait_send()

        @pl.when(on_y(c))
        def _():
            to_y(c, zero).wait_send()

        keep(c).wait()
        for k in range(3):
            max_copy(c, k).wait_send()
        return carry

    lax.fori_loop(0, chunks, settle, 0)
    for copy in tails:
        copy.wait()
    for copy in bank_copies:
        copy.wait_send()
    for k in range(3):
        square_copies[k].wait_send()
        remote(router_buf.at[square[k]], router_buf.at[square[k]], square_send.at[k], square_recv.at[k], square[k]).wait_recv()
    high = router_t.shape[0]
    for z in range(4):
        for b in range(banks):
            router_out[b * high:(b + 1) * high, z * gain.shape[1]:(z + 1) * gain.shape[1]] = router_buf[z, b]

    def last(c, carry):
        forward(c, lambda copy: copy.wait_send())
        remote(narrow.at[c], place(c, pd), send_f.at[c], recv_d.at[c], pd).wait_recv()
        return carry

    lax.fori_loop(0, chunks, last, 0)


def take_kernel(full, scale, router, full_out, scale_out, router_out):
    full_out[...] = full[...]
    scale_out[...] = scale[...]
    router_out[...] = router[...]


def patch_kernel(chunks, rows, tail, from_x, from_y, base, out, x_buf, y_buf, in_sem, out_sem):
    del base
    zero = lax.axis_index("zero")
    px, py, _ = peers_of(zero)
    per, width = out.shape[1] // rows, from_x.shape[2]
    load = [
        pltpu.make_async_copy(src, dst, in_sem.at[k])
        for k, (src, dst) in enumerate(((from_x, x_buf), (from_y, y_buf)))
    ]
    for copy in load:
        copy.start()
    for copy in load:
        copy.wait()
    stores = []
    for n in range(tail):
        c = chunks - tail + n
        buf, owner = (y_buf, py) if c % 2 == 0 else (x_buf, px)
        cols = pl.ds(pl.multiple_of(owner * width, width), width)
        dst = out.at[c // per, pl.ds((c % per) * rows, rows), cols]
        stores.append(pltpu.make_async_copy(buf.at[n // 2], dst, out_sem.at[n]))
        stores[-1].start()
    for copy in stores:
        copy.wait()


def on_square(banks, w_down, avg_down, mix_share, router_weight, router_gain):
    experts, inner, width = w_down.shape
    rows = ROWS
    chunks = experts * inner // rows
    tail = TAIL_EXPERTS * inner // rows
    kind = jnp.bfloat16
    columns, deep = router_weight.shape[1], router_weight.shape[0]
    any_spec = pl.BlockSpec(memory_space=pl.ANY)
    hbm_spec = pl.BlockSpec(memory_space=pltpu.HBM)
    vmem_spec = pl.BlockSpec(memory_space=pltpu.VMEM)
    dma = pltpu.SemaphoreType.DMA
    half_tail = (max(tail // 2, 1), rows, width)
    full, tail_x, tail_y, scale, router = pl.pallas_call(
        functools.partial(exchange_kernel, banks, chunks, rows, tail),
        out_shape=(
            jax.ShapeDtypeStruct((experts, inner, 4 * width), kind),
            jax.ShapeDtypeStruct(half_tail, kind),
            jax.ShapeDtypeStruct(half_tail, kind),
            jax.ShapeDtypeStruct((experts, inner), jnp.float32),
            jax.ShapeDtypeStruct((columns * banks, deep * 4), kind),
        ),
        in_specs=[any_spec, any_spec, pl.BlockSpec(memory_space=pltpu.SMEM), vmem_spec, vmem_spec],
        out_specs=(hbm_spec, hbm_spec, hbm_spec, vmem_spec, vmem_spec),
        scratch_shapes=[
            pltpu.VMEM((IN_SLOTS, rows, width), jnp.float32),
            pltpu.VMEM((IN_SLOTS, rows, width), jnp.float32),
            pltpu.VMEM((2, rows, width), jnp.float32),
            pltpu.VMEM((chunks, rows, width), kind),
            pltpu.VMEM((chunks, rows // LANES, LANES), jnp.float32),
            pltpu.VMEM((3, chunks, rows // LANES, LANES), jnp.float32),
            pltpu.VMEM((chunks, rows // LANES, LANES), jnp.float32),
            pltpu.VMEM((4, banks, columns, deep), kind),
            dma((2, IN_SLOTS)), dma((3, chunks)), dma((3, chunks)),
            dma((chunks,)), dma((chunks,)), dma((chunks,)),
            dma((chunks,)), dma((chunks,)), dma((chunks,)),
            dma((chunks,)), dma((max(tail, 1),)),
            dma((banks - 1,)), dma((banks - 1,)), dma((3,)), dma((3,)),
        ],
        compiler_params=pltpu.CompilerParams(
            collective_id=0, has_side_effects=True, vmem_limit_bytes=40 * 1024 * 1024
        ),
        name="exchange",
    )(w_down, avg_down, mix_share, router_weight.T, router_gain[None, :])

    whole = (1, inner, 4 * width)
    fixed = lambda e: (0, 0)
    if tail:
        to_x = [(z, z ^ 1) for z in range(4)]
        to_y = [(z, z ^ 2) for z in range(4)]
        from_x = lax.ppermute(tail_x, "zero", to_x)
        from_y = lax.ppermute(tail_y, "zero", to_y)
    taken, scale, router = pl.pallas_call(
        take_kernel,
        grid=(experts,),
        out_shape=tuple(jax.ShapeDtypeStruct(v.shape, v.dtype) for v in (full, scale, router)),
        in_specs=[
            pl.BlockSpec(whole, lambda e: (e, 0, 0)),
            pl.BlockSpec(scale.shape, fixed),
            pl.BlockSpec(router.shape, fixed),
        ],
        out_specs=(
            pl.BlockSpec(whole, lambda e: (e, 0, 0)),
            pl.BlockSpec(scale.shape, fixed),
            pl.BlockSpec(router.shape, fixed),
        ),
        cost_estimate=pl.CostEstimate(flops=0, bytes_accessed=4 * full.size, transcendentals=0),
        name="take",
    )(full, scale, router)
    if tail:
        taken = pl.pallas_call(
            functools.partial(patch_kernel, chunks, rows, tail),
            out_shape=jax.ShapeDtypeStruct(taken.shape, taken.dtype),
            in_specs=[any_spec] * 3,
            out_specs=hbm_spec,
            scratch_shapes=[
                pltpu.VMEM(half_tail, kind), pltpu.VMEM(half_tail, kind), dma((2,)), dma((tail,)),
            ],
            input_output_aliases={2: 0},
            cost_estimate=pl.CostEstimate(flops=0, bytes_accessed=4 * from_x.size, transcendentals=0),
            name="patch",
        )(from_x, from_y, taken)
    return taken, scale, router.T


def anywhere(w_down, avg_down, mix_share, router_weight, router_gain):
    fresh_down = mix_share[:, None, None] * w_down + (1.0 - mix_share[:, None, None]) * avg_down
    scale_down = lax.pmax(jnp.max(jnp.abs(fresh_down), axis=2), "zero")
    narrow_down = (fresh_down / jnp.expand_dims(scale_down, 2)).astype(jnp.bfloat16)
    serve_down = lax.all_gather(narrow_down, "zero", axis=2, tiled=True)
    part_router = (router_weight * router_gain[:, None]).astype(jnp.bfloat16)
    row_router = lax.all_gather(part_router, "zero", axis=0, tiled=True)
    serve_router = lax.all_gather(row_router, "bank", axis=1, tiled=True)
    return (serve_down, scale_down, serve_router)


def solution(mesh):
    body = functools.partial(on_square, mesh.shape["bank"]) if mesh.shape["zero"] == 4 else anywhere
    return jax.shard_map(
        body,
        mesh=mesh,
        in_specs=(
            P("bank", None, "zero"),
            P("bank", None, "zero"),
            P("bank"),
            P("zero", "bank"),
            P("zero"),
        ),
        out_specs=(P("bank", None, None), P("bank", None), P()),
        check_vma=False,
    )
```

```python
import functools

import jax
import jax.numpy as jnp
from jax import lax
from jax.experimental import pallas as pl
from jax.experimental.pallas import tpu as pltpu
from jax.sharding import PartitionSpec as P

MESH = pl.DeviceIdType.MESH
LANES = 128
ROWS = 1024
TAIL_EXPERTS = 2
IN_SLOTS = 3
HEAD = 2
FIRST = 1
VMEM_BYTES = 67043328


def peers_of(zero):
    side = lax.rem(zero, 2)
    return zero + 1 - 2 * side, lax.rem(zero + 2, 4), 3 - zero


def exchange_kernel(
    banks, chunks, rows, tail,
    w_hbm, a_hbm, mix_hbm, router_hbm, gain_hbm,
    full, tail_x, tail_y, scale_hbm, router_to,
    mix, router_t, gain, scale_out, router_out, small_sem,
    w_buf, a_buf, fresh, narrow, own_max, peer_max, scales, router_buf,
    in_sem, max_send, max_recv, rest_send, rest_recv, send_x, send_y, send_f, recv_x, recv_y, recv_d,
    keep_sem, tail_sem, bank_send, bank_recv, square_send, square_recv,
):
    zero, bank = lax.axis_index("zero"), lax.axis_index("bank")
    square = peers_of(zero)
    px, py, pd = square
    per = w_hbm.shape[1] // rows
    width = w_hbm.shape[2]
    blocks = rows // LANES
    groups = width // LANES

    def place(c, owner):
        cols = pl.ds(pl.multiple_of(owner * width, width), width)
        return full.at[lax.div(c, per), pl.ds(pl.multiple_of(lax.rem(c, per) * rows, rows), rows), cols]

    def loads(c):
        slot = lax.rem(c, IN_SLOTS)
        piece = (lax.div(c, per), pl.ds(pl.multiple_of(lax.rem(c, per) * rows, rows), rows))
        return (
            pltpu.make_async_copy(w_hbm.at[piece], w_buf.at[slot], in_sem.at[0, slot]),
            pltpu.make_async_copy(a_hbm.at[piece], a_buf.at[slot], in_sem.at[1, slot]),
        )

    def start_loads(c):
        for copy in loads(c):
            copy.start()

    def remote(src, dst, send, recv, to):
        return pltpu.make_async_remote_copy(
            src_ref=src, dst_ref=dst, send_sem=send, recv_sem=recv,
            device_id={"zero": to}, device_id_type=MESH,
        )

    def max_copy(c, k):
        return remote(own_max.at[c], peer_max.at[k, c], max_send.at[k, c], max_recv.at[k, c], square[k])

    def to_x(c, owner):
        return remote(narrow.at[c], place(c, owner), send_x.at[c], recv_x.at[c], px)

    def to_y(c, owner):
        return remote(narrow.at[c], place(c, owner), send_y.at[c], recv_y.at[c], py)

    def on_x(c):
        return (c < chunks - tail) | (lax.rem(c, 2) == 0)

    def on_y(c):
        return (c < chunks - tail) | (lax.rem(c, 2) == 1)

    def keep(c):
        return pltpu.make_async_copy(narrow.at[c], place(c, zero), keep_sem.at[c])

    def mix_stage(c):
        for copy in loads(c):
            copy.wait()

        @pl.when(c + IN_SLOTS - 1 < chunks)
        def _():
            start_loads(c + IN_SLOTS - 1)

        slot = lax.rem(c, IN_SLOTS)
        share = mix[lax.div(c, per)]
        for j in range(blocks):
            part = pl.ds(j * LANES, LANES)
            value = share * w_buf[slot, part, :] + (1.0 - share) * a_buf[slot, part, :]
            fresh[c, part, :] = value
            size = jnp.abs(value)
            top = size[:, :LANES]
            for g in range(1, groups):
                top = jnp.maximum(top, size[:, g * LANES:(g + 1) * LANES])
            own_max[c, pl.ds(j, 1), :] = jnp.max(top.T, axis=0, keepdims=True)

    def send_stage(c):
        scale = jnp.maximum(
            jnp.maximum(own_max[c], peer_max[0, c]), jnp.maximum(peer_max[1, c], peer_max[2, c])
        )
        scales[c] = scale
        inverse = 1.0 / scale
        for j in range(blocks):
            part = pl.ds(j * LANES, LANES)
            column = jnp.broadcast_to(inverse[j:j + 1, :], (LANES, LANES)).T
            for g in range(groups):
                cols = slice(g * LANES, (g + 1) * LANES)
                narrow[c, part, cols] = (fresh[c, part, cols] * column).astype(narrow.dtype)

        @pl.when(on_x(c))
        def _():
            to_x(c, zero).start()

        @pl.when(on_y(c))
        def _():
            to_y(c, zero).start()

        keep(c).start()

    def forward(c, do):
        @pl.when(lax.rem(c, 2) == 0)
        def _():
            do(remote(place(c, px), place(c, px), send_f.at[c], recv_d.at[c], py))

        @pl.when(lax.rem(c, 2) == 1)
        def _():
            do(remote(place(c, py), place(c, py), send_f.at[c], recv_d.at[c], px))

    small = [
        pltpu.make_async_copy(src, dst, small_sem.at[k])
        for k, (src, dst) in enumerate(((mix_hbm, mix), (router_hbm, router_t), (gain_hbm, gain)))
    ]
    small[0].start()
    for c in range(IN_SLOTS - 1):
        start_loads(c)
    for copy in small[1:]:
        copy.start()
    barrier = pltpu.get_barrier_semaphore()
    others = [lax.rem(bank + k, banks) for k in range(1, banks)]
    for to in square:
        pl.semaphore_signal(barrier, inc=1, device_id={"zero": to}, device_id_type=MESH)
    for to in others:
        pl.semaphore_signal(barrier, inc=1, device_id={"bank": to}, device_id_type=MESH)
    pl.semaphore_wait(barrier, 3 + len(others))

    small[0].wait()
    def early(c, carry):
        mix_stage(c)
        for k in range(3):
            max_copy(c, k).start()
        return carry

    def early_send(c, carry):
        for k in range(3):
            max_copy(c, k).wait_recv()
        send_stage(c)
        return carry

    def late(c, carry):
        mix_stage(c)
        return carry

    def late_send(c, carry):
        send_stage(c)
        return carry

    rest = pl.ds(HEAD, chunks - HEAD)
    rest_copies = [
        remote(own_max.at[rest], peer_max.at[k, rest], rest_send.at[k], rest_recv.at[k], square[k])
        for k in range(3)
    ]
    lax.fori_loop(0, HEAD, early, 0)
    lax.fori_loop(0, FIRST, early_send, 0)
    lax.fori_loop(HEAD, chunks, late, 0)
    for copy in rest_copies:
        copy.start()
    lax.fori_loop(FIRST, HEAD, early_send, 0)
    for copy in rest_copies:
        copy.wait_recv()
    lax.fori_loop(HEAD, chunks, late_send, 0)

    tails = []
    for n in range(tail):
        c = chunks - tail + n
        out = tail_y if c % 2 == 0 else tail_x
        tails.append(pltpu.make_async_copy(narrow.at[c], out.at[n // 2], tail_sem.at[n]))
        tails[-1].start()

    for copy in small[1:]:
        copy.wait()
    router_buf[zero, bank] = (router_t[...] * gain[...]).astype(router_buf.dtype)
    bank_copies = [
        pltpu.make_async_remote_copy(
            src_ref=router_buf.at[zero, bank], dst_ref=router_buf.at[zero, bank],
            send_sem=bank_send.at[k], recv_sem=bank_recv.at[k],
            device_id={"bank": to}, device_id_type=MESH,
        )
        for k, to in enumerate(others)
    ]
    for copy in bank_copies:
        copy.start()
    for k in range(len(others)):
        source = lax.rem(bank + banks - k - 1, banks)
        pltpu.make_async_remote_copy(
            src_ref=router_buf.at[zero, source], dst_ref=router_buf.at[zero, source],
            send_sem=bank_send.at[k], recv_sem=bank_recv.at[k],
            device_id={"bank": others[k]}, device_id_type=MESH,
        ).wait_recv()
    square_copies = [
        remote(router_buf.at[zero], router_buf.at[zero], square_send.at[k], square_recv.at[k], square[k])
        for k in range(3)
    ]
    for copy in square_copies:
        copy.start()

    def relay(c, carry):
        @pl.when(lax.rem(c, 2) == 0)
        def _():
            to_x(c, px).wait_recv()

        @pl.when(lax.rem(c, 2) == 1)
        def _():
            to_y(c, py).wait_recv()

        forward(c, lambda copy: copy.start())
        return carry

    lax.fori_loop(0, chunks, relay, 0)

    for c in range(chunks):
        scale_out[c // per:c // per + 1, pl.ds((c % per) * rows, rows)] = jnp.concatenate(
            [scales[c, j:j + 1, :] for j in range(blocks)], axis=1
        )

    scale_copy = pltpu.make_async_copy(scale_out, scale_hbm, small_sem.at[3])
    scale_copy.start()

    def settle(c, carry):
        @pl.when((lax.rem(c, 2) == 1) & (c < chunks - tail))
        def _():
            to_x(c, px).wait_recv()

        @pl.when((lax.rem(c, 2) == 0) & (c < chunks - tail))
        def _():
            to_y(c, py).wait_recv()

        @pl.when(on_x(c))
        def _():
            to_x(c, zero).wait_send()

        @pl.when(on_y(c))
        def _():
            to_y(c, zero).wait_send()

        keep(c).wait()
        return carry

    lax.fori_loop(0, chunks, settle, 0)
    for c in range(HEAD):
        for k in range(3):
            max_copy(c, k).wait_send()
    for copy in rest_copies:
        copy.wait_send()
    for copy in tails:
        copy.wait()
    for copy in bank_copies:
        copy.wait_send()
    for k in range(3):
        square_copies[k].wait_send()
        remote(router_buf.at[square[k]], router_buf.at[square[k]], square_send.at[k], square_recv.at[k], square[k]).wait_recv()
    high = router_t.shape[0]
    for z in range(4):
        for b in range(banks):
            router_out[b * high:(b + 1) * high, z * gain.shape[1]:(z + 1) * gain.shape[1]] = router_buf[z, b]

    router_copy = pltpu.make_async_copy(router_out, router_to, small_sem.at[4])
    router_copy.start()

    def last(c, carry):
        forward(c, lambda copy: copy.wait_send())
        remote(narrow.at[c], place(c, pd), send_f.at[c], recv_d.at[c], pd).wait_recv()
        return carry

    lax.fori_loop(0, chunks, last, 0)
    scale_copy.wait()
    router_copy.wait()


def take_kernel(full, scale, router, full_out, scale_out, router_out):
    full_out[...] = full[...]
    scale_out[...] = scale[...]
    router_out[...] = router[...]


def patch_kernel(chunks, rows, tail, from_x, from_y, base, out, buf, in_sem, out_sem):
    del base
    zero = lax.axis_index("zero")
    px, py, _ = peers_of(zero)
    per, width = out.shape[1] // rows, from_x.shape[2]
    loads, stores = [], []
    for n in range(tail):
        c = chunks - tail + n
        src, owner = (from_y, py) if c % 2 == 0 else (from_x, px)
        loads.append(pltpu.make_async_copy(src.at[n // 2], buf.at[n], in_sem.at[n]))
        cols = pl.ds(pl.multiple_of(owner * width, width), width)
        dst = out.at[c // per, pl.ds((c % per) * rows, rows), cols]
        stores.append(pltpu.make_async_copy(buf.at[n], dst, out_sem.at[n]))
    for load in loads:
        load.start()
    for load, store in zip(loads, stores):
        load.wait()
        store.start()
    for store in stores:
        store.wait()


def on_square(banks, w_down, avg_down, mix_share, router_weight, router_gain):
    experts, inner, width = w_down.shape
    rows = ROWS
    chunks = experts * inner // rows
    tail = TAIL_EXPERTS * inner // rows
    kind = jnp.bfloat16
    columns, deep = router_weight.shape[1], router_weight.shape[0]
    any_spec = pl.BlockSpec(memory_space=pl.ANY)
    hbm_spec = pl.BlockSpec(memory_space=pltpu.HBM)
    dma = pltpu.SemaphoreType.DMA
    half_tail = (max(tail // 2, 1), rows, width)
    full, tail_x, tail_y, scale, router = pl.pallas_call(
        functools.partial(exchange_kernel, banks, chunks, rows, tail),
        out_shape=(
            jax.ShapeDtypeStruct((experts, inner, 4 * width), kind),
            jax.ShapeDtypeStruct(half_tail, kind),
            jax.ShapeDtypeStruct(half_tail, kind),
            jax.ShapeDtypeStruct((experts, inner), jnp.float32),
            jax.ShapeDtypeStruct((columns * banks, deep * 4), kind),
        ),
        in_specs=[any_spec] * 5,
        out_specs=(hbm_spec,) * 5,
        scratch_shapes=[
            pltpu.SMEM(mix_share.shape, jnp.float32),
            pltpu.VMEM((columns, deep), jnp.float32),
            pltpu.VMEM((1, deep), jnp.float32),
            pltpu.VMEM((experts, inner), jnp.float32),
            pltpu.VMEM((columns * banks, deep * 4), kind),
            dma((5,)),
            pltpu.VMEM((IN_SLOTS, rows, width), jnp.float32),
            pltpu.VMEM((IN_SLOTS, rows, width), jnp.float32),
            pltpu.VMEM((chunks, rows, width), jnp.float32),
            pltpu.VMEM((chunks, rows, width), kind),
            pltpu.VMEM((chunks, rows // LANES, LANES), jnp.float32),
            pltpu.VMEM((3, chunks, rows // LANES, LANES), jnp.float32),
            pltpu.VMEM((chunks, rows // LANES, LANES), jnp.float32),
            pltpu.VMEM((4, banks, columns, deep), kind),
            dma((2, IN_SLOTS)), dma((3, HEAD)), dma((3, HEAD)), dma((3,)), dma((3,)),
            dma((chunks,)), dma((chunks,)), dma((chunks,)),
            dma((chunks,)), dma((chunks,)), dma((chunks,)),
            dma((chunks,)), dma((max(tail, 1),)),
            dma((banks - 1,)), dma((banks - 1,)), dma((3,)), dma((3,)),
        ],
        compiler_params=pltpu.CompilerParams(
            collective_id=0, has_side_effects=True, vmem_limit_bytes=VMEM_BYTES
        ),
        name="exchange",
    )(w_down, avg_down, mix_share, router_weight.T, router_gain[None, :])

    whole = (1, inner, 4 * width)
    fixed = lambda e: (0, 0)
    if tail:
        to_x = [(z, z ^ 1) for z in range(4)]
        to_y = [(z, z ^ 2) for z in range(4)]
        from_x = lax.ppermute(tail_x, "zero", to_x)
        from_y = lax.ppermute(tail_y, "zero", to_y)
    taken, scale, router = pl.pallas_call(
        take_kernel,
        grid=(experts,),
        out_shape=tuple(jax.ShapeDtypeStruct(v.shape, v.dtype) for v in (full, scale, router)),
        in_specs=[
            pl.BlockSpec(whole, lambda e: (e, 0, 0)),
            pl.BlockSpec(scale.shape, fixed),
            pl.BlockSpec(router.shape, fixed),
        ],
        out_specs=(
            pl.BlockSpec(whole, lambda e: (e, 0, 0)),
            pl.BlockSpec(scale.shape, fixed),
            pl.BlockSpec(router.shape, fixed),
        ),
        cost_estimate=pl.CostEstimate(flops=0, bytes_accessed=4 * full.size, transcendentals=0),
        compiler_params=pltpu.CompilerParams(vmem_limit_bytes=VMEM_BYTES),
        name="take",
    )(full, scale, router)
    if tail:
        taken = pl.pallas_call(
            functools.partial(patch_kernel, chunks, rows, tail),
            out_shape=jax.ShapeDtypeStruct(taken.shape, taken.dtype),
            in_specs=[any_spec] * 3,
            out_specs=hbm_spec,
            scratch_shapes=[pltpu.VMEM((tail, rows, width), kind), dma((tail,)), dma((tail,))],
            input_output_aliases={2: 0},
            cost_estimate=pl.CostEstimate(flops=0, bytes_accessed=4 * from_x.size, transcendentals=0),
            compiler_params=pltpu.CompilerParams(vmem_limit_bytes=VMEM_BYTES),
            name="patch",
        )(from_x, from_y, taken)
    return taken, scale, router.T


def anywhere(w_down, avg_down, mix_share, router_weight, router_gain):
    fresh_down = mix_share[:, None, None] * w_down + (1.0 - mix_share[:, None, None]) * avg_down
    scale_down = lax.pmax(jnp.max(jnp.abs(fresh_down), axis=2), "zero")
    narrow_down = (fresh_down / jnp.expand_dims(scale_down, 2)).astype(jnp.bfloat16)
    serve_down = lax.all_gather(narrow_down, "zero", axis=2, tiled=True)
    part_router = (router_weight * router_gain[:, None]).astype(jnp.bfloat16)
    row_router = lax.all_gather(part_router, "zero", axis=0, tiled=True)
    serve_router = lax.all_gather(row_router, "bank", axis=1, tiled=True)
    return (serve_down, scale_down, serve_router)


def solution(mesh):
    body = functools.partial(on_square, mesh.shape["bank"]) if mesh.shape["zero"] == 4 else anywhere
    return jax.shard_map(
        body,
        mesh=mesh,
        in_specs=(
            P("bank", None, "zero"),
            P("bank", None, "zero"),
            P("bank"),
            P("zero", "bank"),
            P("zero"),
        ),
        out_specs=(P("bank", None, None), P("bank", None), P()),
        check_vma=False,
    )
```
